32 devices in a mesh: row: 4 (over x, core), col: 4 (over z), layer: 2 (over y).
Axes of the slice: x: 2, y: 2, z: 4, core: 2. Of those that a mesh axis runs over, the one named last changes fastest.
Arguments:
- attn_values: bfloat16 [2048, 8192], P('row', ('layer', 'col')), may hold values from -6 to 6
- out_weight: bfloat16 [8192, 8192], P(('layer', 'row'), 'col'), may hold values from -0.09375 to 0.09375
Outputs:
- projected: bfloat16 [2048, 8192], P('row', ('col', 'layer'))
The draws below stay inside these ranges and needn't reach their ends.
All inputs are finite; a program needn't handle non-finite values.
Results may differ from the reference program's by a relative error of at most 0.001.
Values may be sent and summed in bfloat16 or wider, within the bound.
A program may use at most 128 MiB of HBM per device.

```python
import jax
import jax.numpy as jnp
from jax import lax

D = 8192
TOK_DEV = 512
TOKENS = 2048
N_ROW = 4


def with_spikes(entries, own_key, source, target, parts, factor):
    owner, partner = [(jnp.arange(entries.shape[axis_at]) // (entries.shape[axis_at] // parts)).reshape([-1 if axis == axis_at else 1 for axis in range(entries.ndim)]) for axis_at in (source, target)]
    chosen = jax.random.permutation(own_key, parts)[partner]
    strong = (owner == chosen) | (owner == (partner + parts // 2) % parts)
    return jnp.where(strong, factor * entries, entries)


def levels(stream_key, extent, pieces, low, high):
    loudness, own = 1.0, jax.random.fold_in(stream_key, 6)
    for axis_at, blocks in pieces:
        heights = jnp.exp(jax.random.uniform(jax.random.fold_in(own, axis_at), (blocks,), jnp.float32, low / len(pieces), high / len(pieces)))
        loudness = loudness * jnp.repeat(heights, extent[axis_at] // blocks).reshape([-1 if axis == axis_at else 1 for axis in range(len(extent))])
    return loudness


def noise(rng, dims, spread, bound, cuts=(), kind=jnp.bfloat16):
    loudness = levels(rng, dims, cuts, -0.22, 0.18) if cuts else 1.0
    entries = jax.random.normal(rng, dims, jnp.float32) * spread * loudness
    return jnp.minimum(jnp.maximum(entries, -bound), bound).astype(kind)


def bell_draw_with(rng, dims, spread, bound, shards, heavy, held_as=jnp.bfloat16):
    array = spread * jax.random.normal(rng, dims, jnp.float32)
    if shards:
        array = array * levels(rng, dims, shards, -0.22, 0.18)
    return jnp.clip(with_spikes(array, jax.random.fold_in(rng, 3), *heavy), -bound, bound).astype(held_as)


def setup_inputs(seed: int = 0) -> dict:
    seeds = jax.random.split(jax.random.key(seed), 3)
    return {
        "attn_values": noise(seeds[0], (TOKENS, D), 1.0, 6.0, ((0, 4), (1, 8))),
        "out_weight": bell_draw_with(seeds[1], (D, D), D ** -0.5, 0.09375, ((0, 8), (1, 4)), (0, 1, 8, 2.0)),
    }


def reference(attn_values, out_weight):
    token_blocks = attn_values.reshape(N_ROW, TOK_DEV, D)
    half_depth = D // 2

    def project(block):
        lower_part = jnp.dot(block[:, :half_depth], out_weight[:half_depth], preferred_element_type=jnp.float32)
        upper_part = jnp.dot(block[:, half_depth:], out_weight[half_depth:], preferred_element_type=jnp.float32)
        return (lower_part + upper_part).astype(jnp.bfloat16)

    return lax.map(project, token_blocks).reshape(TOK_DEV * N_ROW, D)
```

```python
import functools

import jax
import jax.numpy as jnp
from jax import lax
from jax.experimental import pallas as pl
from jax.experimental.pallas import tpu as pltpu
from jax.sharding import PartitionSpec as P

TOKEN_CHUNKS = 4
COLUMN_CHUNKS = 8


def schedule(token_chunks, column_chunks, col_count):
    events = []
    for t in range(token_chunks):
        for d in range(1, col_count):
            at = (col_count - 1) * t + (1 if d == 1 else d + 1)
            events.append((at, 0, t, d))
    span = (col_count - 1) * token_chunks * 4 / 3
    for j in range(column_chunks):
        events.append((span * (j + 1) / column_chunks, 1, j, 0))
    ordered, clock = [], 0
    for at, kind, first, second in sorted(events, key=lambda e: (e[1], e[2], e[3])):
        if kind == 0:
            clock = max(clock, at)
            at = clock
        ordered.append((at, kind, first, second))
    return sorted(ordered)


def kernel(rows, cols, a_ref, w_ref, o_ref, abuf, wbuf, ysend, yrecv, loc_a, loc_w, a_recv, a_right, a_left, w_recv, w_send, p_send, y_recv, y_send):
    r, c, l = lax.axis_index("row"), lax.axis_index("col"), lax.axis_index("layer")
    groups = rows // 2
    core, group = lax.rem(r, 2), r // 2
    partner = 2 * group + 1 - core
    tokens, depth_a = a_ref.shape
    depth_w, width = w_ref.shape
    tt, half = tokens // TOKEN_CHUNKS, width // 2
    nc, jh = width // COLUMN_CHUNKS, COLUMN_CHUNKS // 2

    def peer(g):
        return 2 * lax.rem(group + g + groups, groups) + core

    def a_at(block, t):
        return abuf.at[block, pl.ds(t * tt, tt), :]

    def w_at(row, j):
        return wbuf.at[j, pl.ds(pl.multiple_of(row * depth_w, depth_w), depth_w), :]

    def own_a(t):
        return pltpu.make_async_copy(a_ref.at[pl.ds(t * tt, tt), :], a_at(c, t), loc_a.at[t])

    def own_w(j):
        side = 1 - l if j < jh else l
        at = pl.multiple_of(side * half + (j % jh) * nc, nc)
        return pltpu.make_async_copy(w_ref.at[:, pl.ds(at, nc)], w_at(r, j), loc_w.at[j])

    def a_copy(block, t, to, sems):
        return pltpu.make_async_remote_copy(a_at(block, t), a_at(block, t), sems.at[t, block], a_recv.at[t, block], device_id={"col": to})

    def w_copy(row, j, to, sem):
        return pltpu.make_async_remote_copy(w_at(row, j), w_at(row, j), sem, w_recv.at[j, row], device_id={"row": to})

    def y_copy(t, j):
        rows_t = pl.ds(t * tt, tt)
        return pltpu.make_async_remote_copy(ysend.at[j, rows_t, :], yrecv.at[j, rows_t, :], y_send.at[t, j], y_recv.at[t, j], device_id={"layer": 1 - l})

    def right(block, t):
        return a_copy(block, t, c + 1, a_right)

    def left(block, t):
        return a_copy(block, t, c - 1, a_left)

    for n in range(max(TOKEN_CHUNKS, COLUMN_CHUNKS)):
        if n < TOKEN_CHUNKS:
            own_a(n).start()
        if n < COLUMN_CHUNKS:
            own_w(n).start()

    has_right, has_left = c < cols - 1, c > 0
    barrier = pltpu.get_barrier_semaphore()

    def greet(device_id):
        pl.semaphore_signal(barrier, inc=1, device_id=device_id)

    greet({"row": partner})
    greet({"layer": 1 - l})
    for g in range(1, groups):
        greet({"row": peer(g)})
    pl.when(has_right)(lambda: greet({"col": c + 1}))
    pl.when(has_left)(lambda: greet({"col": c - 1}))
    pl.semaphore_wait(barrier, 1 + groups + has_right.astype(jnp.int32) + has_left.astype(jnp.int32))

    def send_a(t):
        own_a(t).wait()
        pl.when(has_right)(lambda: right(c, t).start())
        pl.when(has_left)(lambda: left(c, t).start())

    def send_w(j):
        own_w(j).wait()
        for g in range(1, groups):
            w_copy(r, j, peer(g), w_send.at[j, g]).start()
        w_copy(r, j, partner, p_send.at[j, 0]).start()

    send_a(0)
    send_w(0)
    send_a(1)
    for j in range(1, COLUMN_CHUNKS):
        send_w(j)

    def take_a(t, d):
        @pl.when(c >= d)
        def _():
            right(c - d, t).wait_recv()
            pl.when(has_right)(lambda: right(c - d, t).start())

        @pl.when(c + d < cols)
        def _():
            left(c + d, t).wait_recv()
            pl.when(has_left)(lambda: left(c + d, t).start())

        if d == cols - 1 and t + 2 < TOKEN_CHUNKS:
            send_a(t + 2)

    def take_w(j):
        for g in range(1, groups):
            source = peer(-g)
            w_copy(source, j, partner, p_send.at[j, g]).wait_recv()
            w_copy(source, j, partner, p_send.at[j, g]).start()

    def take_partner(j):
        for g in range(groups):
            source = 2 * g + 1 - core
            w_copy(source, j, partner, p_send.at[j, 0]).wait_recv()

    def product(rows_t, j):
        total = jnp.dot(abuf[0, rows_t, :], wbuf[j, pl.ds(0, depth_a), :], preferred_element_type=jnp.float32)
        for block in range(1, cols):
            total += jnp.dot(abuf[block, rows_t, :], wbuf[j, pl.ds(block * depth_a, depth_a), :], preferred_element_type=jnp.float32)
        return total

    def partials(tiles):
        t0, j0 = tiles[0]
        wide = 1 + tiles[-1][1] - j0

        def one(n, carry):
            t, j = t0 + n // wide, j0 + lax.rem(n, wide)
            rows_t = pl.ds(pl.multiple_of(t * tt, tt), tt)
            ysend[j, rows_t, :] = product(rows_t, j)
            return carry

        def send(n, carry):
            y_copy(t0 + n // wide, j0 + lax.rem(n, wide)).start()
            return carry

        lax.fori_loop(0, len(tiles), one, 0)
        lax.fori_loop(0, len(tiles), send, 0)

    def finish(j):
        def one(t, carry):
            rows_t = pl.ds(pl.multiple_of(t * tt * 2, tt * 2), tt * 2)
            y_copy(2 * t, j - jh).wait_recv()
            y_copy(2 * t + 1, j - jh).wait_recv()
            o_ref[rows_t, (j - jh) * nc:(j - jh + 1) * nc] = (product(rows_t, j) + yrecv[j - jh, rows_t, :]).astype(o_ref.dtype)
            return carry

        lax.fori_loop(0, TOKEN_CHUNKS // 2, one, 0)

    got_t, got_j, done_own = 0, 0, jh
    for _, kind, first, second in schedule(TOKEN_CHUNKS, COLUMN_CHUNKS, cols):
        if kind == 0:
            take_a(first, second)
            if second == cols - 1:
                got_t = first + 1
                if got_j:
                    partials([(first, j) for j in range(min(got_j, jh))])
        else:
            take_w(first)
            take_partner(first)
            got_j = first + 1
            if first < jh and got_t:
                partials([(t, first) for t in range(got_t)])
        while got_t == TOKEN_CHUNKS and done_own < got_j:
            finish(done_own)
            done_own += 1

    for t in range(TOKEN_CHUNKS):
        for block in range(cols):
            @pl.when(has_right & (block <= c))
            def _():
                right(block, t).wait_send()

            @pl.when(has_left & (block >= c))
            def _():
                left(block, t).wait_send()

        for j in range(jh):
            y_copy(t, j).wait_send()
    for j in range(COLUMN_CHUNKS):
        for g in range(groups):
            w_copy(r, j, partner, p_send.at[j, g]).wait_send()
            if g:
                w_copy(r, j, partner, w_send.at[j, g]).wait_send()


def solution(mesh):
    rows, cols = mesh.shape["row"], mesh.shape["col"]

    def shards(attn_values, out_weight):
        tokens, depth_a = attn_values.shape
        depth_w, width = out_weight.shape
        nc, jh = width // COLUMN_CHUNKS, COLUMN_CHUNKS // 2
        dma = pltpu.SemaphoreType.DMA
        return pl.pallas_call(
            functools.partial(kernel, rows, cols),
            out_shape=jax.ShapeDtypeStruct((tokens, width // 2), jnp.bfloat16),
            in_specs=[pl.BlockSpec(memory_space=pl.ANY)] * 2,
            out_specs=pl.BlockSpec(memory_space=pltpu.VMEM),
            scratch_shapes=[
                pltpu.VMEM((cols, tokens, depth_a), jnp.bfloat16),
                pltpu.VMEM((COLUMN_CHUNKS, rows * depth_w, nc), jnp.bfloat16),
                pltpu.VMEM((jh, tokens, nc), jnp.float32),
                pltpu.VMEM((jh, tokens, nc), jnp.float32),
                dma((TOKEN_CHUNKS,)),
                dma((COLUMN_CHUNKS,)),
                dma((TOKEN_CHUNKS, cols)),
                dma((TOKEN_CHUNKS, cols)),
                dma((TOKEN_CHUNKS, cols)),
                dma((COLUMN_CHUNKS, rows)),
                dma((COLUMN_CHUNKS, rows // 2)),
                dma((COLUMN_CHUNKS, rows // 2)),
                dma((TOKEN_CHUNKS, jh)),
                dma((TOKEN_CHUNKS, jh)),
            ],
            compiler_params=pltpu.CompilerParams(collective_id=0, has_side_effects=True, vmem_limit_bytes=48 * 2**20),
        )(attn_values, out_weight)

    in_specs = (P("row", ("layer", "col")), P(("layer", "row"), "col"))
    out_specs = P("row", ("col", "layer"))
    return jax.shard_map(shards, mesh=mesh, in_specs=in_specs, out_specs=out_specs, check_vma=False)
```

```python
import functools

import jax
import jax.numpy as jnp
from jax import lax
from jax.experimental import pallas as pl
from jax.experimental.pallas import tpu as pltpu
from jax.sharding import PartitionSpec as P

TOKEN_CHUNKS = 4
COLUMN_CHUNKS = 8


def last_pieces(depth_w):
    return max(1, min(4, depth_w // 256))


def schedule(token_chunks, column_chunks, col_count):
    events = []
    for t in range(token_chunks):
        for d in range(1, col_count):
            at = (col_count - 1) * t + (1 if d == 1 else d + 1)
            events.append((at, 0, t, d))
    span = (col_count - 1) * token_chunks * 4 / 3
    for j in range(column_chunks - 1):
        events.append((span * (j + 1) / column_chunks, 1, j, 0))
    ordered, clock = [], 0
    for at, kind, first, second in sorted(events, key=lambda e: (e[1], e[2], e[3])):
        if kind == 0:
            clock = max(clock, at)
            at = clock
        ordered.append((at, kind, first, second))
    return sorted(ordered)


def kernel(rows, cols, a_ref, w_ref, o_ref, abuf, wbuf, ysend, yrecv, early, loc_a, loc_w, a_recv, a_right, a_left, w_recv, w_send, p_send, y_recv, y_send):
    r, c, l = lax.axis_index("row"), lax.axis_index("col"), lax.axis_index("layer")
    groups = rows // 2
    core, group = lax.rem(r, 2), r // 2
    partner = 2 * group + 1 - core
    tokens, depth_a = a_ref.shape
    depth_w, width = w_ref.shape
    tt, half = tokens // TOKEN_CHUNKS, width // 2
    nc, jh = width // COLUMN_CHUNKS, COLUMN_CHUNKS // 2
    last, cuts = COLUMN_CHUNKS - 1, last_pieces(depth_w)
    pieces = last + cuts

    def piece(p):
        return (p, 0, depth_w) if p < last else (last, (p - last) * depth_w // cuts, depth_w // cuts)

    def peer(g):
        return 2 * lax.rem(group + g + groups, groups) + core

    def a_at(block, t):
        return abuf.at[block, pl.ds(t * tt, tt), :]

    def w_at(row, p):
        j, start, count = piece(p)
        return wbuf.at[j, pl.ds(pl.multiple_of(row * depth_w + start, count), count), :]

    def own_a(t):
        return pltpu.make_async_copy(a_ref.at[pl.ds(t * tt, tt), :], a_at(c, t), loc_a.at[t])

    def own_w(p):
        j, start, count = piece(p)
        side = 1 - l if j < jh else l
        at = pl.multiple_of(side * half + (j % jh) * nc, nc)
        return pltpu.make_async_copy(w_ref.at[pl.ds(start, count), pl.ds(at, nc)], w_at(r, p), loc_w.at[p])

    def a_copy(block, t, to, sems):
        return pltpu.make_async_remote_copy(a_at(block, t), a_at(block, t), sems.at[t, block], a_recv.at[t, block], device_id={"col": to})

    def w_copy(row, j, to, sem):
        return pltpu.make_async_remote_copy(w_at(row, j), w_at(row, j), sem, w_recv.at[j, row], device_id={"row": to})

    def y_copy(t, j):
        rows_t = pl.ds(t * tt, tt)
        return pltpu.make_async_remote_copy(ysend.at[j, rows_t, :], yrecv.at[j, rows_t, :], y_send.at[t, j], y_recv.at[t, j], device_id={"layer": 1 - l})

    def right(block, t):
        return a_copy(block, t, c + 1, a_right)

    def left(block, t):
        return a_copy(block, t, c - 1, a_left)

    for n in range(max(TOKEN_CHUNKS, pieces)):
        if n < pieces:
            own_w(n).start()
        if n < TOKEN_CHUNKS:
            own_a(n).start()

    has_right, has_left = c < cols - 1, c > 0
    barrier = pltpu.get_barrier_semaphore()

    def greet(device_id):
        pl.semaphore_signal(barrier, inc=1, device_id=device_id)

    greet({"row": partner})
    greet({"layer": 1 - l})
    for g in range(1, groups):
        greet({"row": peer(g)})
    pl.when(has_right)(lambda: greet({"col": c + 1}))
    pl.when(has_left)(lambda: greet({"col": c - 1}))
    pl.semaphore_wait(barrier, 1 + groups + has_right.astype(jnp.int32) + has_left.astype(jnp.int32))

    def send_a(t):
        own_a(t).wait()
        pl.when(has_right)(lambda: right(c, t).start())
        pl.when(has_left)(lambda: left(c, t).start())

    def send_w(j):
        own_w(j).wait()
        for g in range(1, groups):
            w_copy(r, j, peer(g), w_send.at[j, g]).start()
        w_copy(r, j, partner, p_send.at[j, 0]).start()

    send_w(0)
    send_a(0)
    send_a(1)
    for p in range(1, pieces):
        send_w(p)

    def take_a(t, d):
        @pl.when(c >= d)
        def _():
            right(c - d, t).wait_recv()
            pl.when(has_right)(lambda: right(c - d, t).start())

        @pl.when(c + d < cols)
        def _():
            left(c + d, t).wait_recv()
            pl.when(has_left)(lambda: left(c + d, t).start())

        if d == cols - 1 and t + 2 < TOKEN_CHUNKS:
            send_a(t + 2)

    def take_w(j):
        for g in range(1, groups):
            source = peer(-g)
            w_copy(source, j, partner, p_send.at[j, g]).wait_recv()
            w_copy(source, j, partner, p_send.at[j, g]).start()

    def take_partner(j):
        for g in range(groups):
            source = 2 * g + 1 - core
            w_copy(source, j, partner, p_send.at[j, 0]).wait_recv()

    def product(rows_t, j):
        total = jnp.dot(abuf[0, rows_t, :], wbuf[j, pl.ds(0, depth_a), :], preferred_element_type=jnp.float32)
        for block in range(1, cols):
            total += jnp.dot(abuf[block, rows_t, :], wbuf[j, pl.ds(block * depth_a, depth_a), :], preferred_element_type=jnp.float32)
        return total

    def partials(tiles):
        t0, j0 = tiles[0]
        wide = 1 + tiles[-1][1] - j0

        def one(n, carry):
            t, j = t0 + n // wide, j0 + lax.rem(n, wide)
            rows_t = pl.ds(pl.multiple_of(t * tt, tt), tt)
            ysend[j, rows_t, :] = product(rows_t, j)
            return carry

        def send(n, carry):
            y_copy(t0 + n // wide, j0 + lax.rem(n, wide)).start()
            return carry

        lax.fori_loop(0, len(tiles), one, 0)
        lax.fori_loop(0, len(tiles), send, 0)

    def finish(j):
        def one(t, carry):
            rows_t = pl.ds(pl.multiple_of(t * tt * 2, tt * 2), tt * 2)
            y_copy(2 * t, j - jh).wait_recv()
            y_copy(2 * t + 1, j - jh).wait_recv()
            o_ref[rows_t, (j - jh) * nc:(j - jh + 1) * nc] = (product(rows_t, j) + yrecv[j - jh, rows_t, :]).astype(o_ref.dtype)
            return carry

        lax.fori_loop(0, TOKEN_CHUNKS // 2, one, 0)

    def part(j, rows_t, start, count):
        columns = pl.ds(pl.multiple_of(lax.rem(start, depth_a), min(count, depth_a)), count)
        weights = wbuf[j, pl.ds(pl.multiple_of(start, count), count), :]
        return jnp.dot(abuf[start // depth_a, rows_t, columns], weights, preferred_element_type=jnp.float32)

    def each_rows(body):
        def one(t, carry):
            body(pl.ds(pl.multiple_of(t * tt * 2, tt * 2), tt * 2))
            return carry

        lax.fori_loop(0, TOKEN_CHUNKS // 2, one, 0)

    def take_own_rows():
        for h in range(cuts):
            w_copy(partner, last + h, partner, p_send.at[last + h, 0]).wait_recv()
        count = min(depth_w, depth_a)
        for n in range(depth_w // count):
            @each_rows
            def _(rows_t):
                total = part(last, rows_t, r * depth_w + n * count, count) + part(last, rows_t, partner * depth_w + n * count, count)
                early[rows_t, :] = total if n == 0 else early[rows_t, :] + total

    def finish_last():
        count = depth_w // cuts
        for t in range(TOKEN_CHUNKS):
            y_copy(t, jh - 1).wait_recv()
        for h in range(cuts):
            take_w(last + h)
            for g in range(1, groups):
                own, other = peer(-g), peer(-g) + 1 - 2 * core

                @each_rows
                def _(rows_t):
                    early[rows_t, :] += part(last, rows_t, own * depth_w + h * count, count)

                w_copy(other, last + h, partner, p_send.at[last + h, 0]).wait_recv()

                @each_rows
                def _(rows_t):
                    total = early[rows_t, :] + part(last, rows_t, other * depth_w + h * count, count)
                    if h < cuts - 1 or g < groups - 1:
                        early[rows_t, :] = total
                    else:
                        o_ref[rows_t, (jh - 1) * nc:jh * nc] = (total + yrecv[jh - 1, rows_t, :]).astype(o_ref.dtype)

    got_t, got_j, done_own, own_rows = 0, 0, jh, False
    for _, kind, first, second in schedule(TOKEN_CHUNKS, COLUMN_CHUNKS, cols):
        if kind == 0:
            take_a(first, second)
            if second == cols - 1:
                got_t = first + 1
                if got_j:
                    partials([(first, j) for j in range(min(got_j, jh))])
        else:
            if first == last - 1 and got_t == TOKEN_CHUNKS:
                take_own_rows()
                own_rows = True
            take_w(first)
            take_partner(first)
            got_j = first + 1
            if first < jh and got_t:
                partials([(t, first) for t in range(got_t)])
        while got_t == TOKEN_CHUNKS and done_own < got_j:
            finish(done_own)
            done_own += 1
    if not own_rows:
        take_own_rows()
    finish_last()

    for t in range(TOKEN_CHUNKS):
        for block in range(cols):
            @pl.when(has_right & (block <= c))
            def _():
                right(block, t).wait_send()

            @pl.when(has_left & (block >= c))
            def _():
                left(block, t).wait_send()

        for j in range(jh):
            y_copy(t, j).wait_send()
    for p in range(pieces):
        for g in range(groups):
            w_copy(r, p, partner, p_send.at[p, g]).wait_send()
            if g:
                w_copy(r, p, partner, w_send.at[p, g]).wait_send()


def solution(mesh):
    rows, cols = mesh.shape["row"], mesh.shape["col"]

    def shards(attn_values, out_weight):
        tokens, depth_a = attn_values.shape
        depth_w, width = out_weight.shape
        nc, jh = width // COLUMN_CHUNKS, COLUMN_CHUNKS // 2
        pieces = COLUMN_CHUNKS - 1 + last_pieces(depth_w)
        dma = pltpu.SemaphoreType.DMA
        return pl.pallas_call(
            functools.partial(kernel, rows, cols),
            out_shape=jax.ShapeDtypeStruct((tokens, width // 2), jnp.bfloat16),
            in_specs=[pl.BlockSpec(memory_space=pltpu.HBM)] * 2,
            out_specs=pl.BlockSpec(memory_space=pltpu.VMEM),
            scratch_shapes=[
                pltpu.VMEM((cols, tokens, depth_a), jnp.bfloat16),
                pltpu.VMEM((COLUMN_CHUNKS, rows * depth_w, nc), jnp.bfloat16),
                pltpu.VMEM((jh, tokens, nc), jnp.float32),
                pltpu.VMEM((jh, tokens, nc), jnp.float32),
                pltpu.VMEM((tokens, nc), jnp.float32),
                dma((TOKEN_CHUNKS,)),
                dma((pieces,)),
                dma((TOKEN_CHUNKS, cols)),
                dma((TOKEN_CHUNKS, cols)),
                dma((TOKEN_CHUNKS, cols)),
                dma((pieces, rows)),
                dma((pieces, rows // 2)),
                dma((pieces, rows // 2)),
                dma((TOKEN_CHUNKS, jh)),
                dma((TOKEN_CHUNKS, jh)),
            ],
            compiler_params=pltpu.CompilerParams(collective_id=0, has_side_effects=True, vmem_limit_bytes=48 * 2**20),
        )(*(pltpu.with_memory_space_constraint(x, pltpu.HBM) for x in (attn_values, out_weight)))

    in_specs = (P("row", ("layer", "col")), P(("layer", "row"), "col"))
    out_specs = P("row", ("col", "layer"))
    return jax.shard_map(shards, mesh=mesh, in_specs=in_specs, out_specs=out_specs, check_vma=False)
```

```python
import functools

import jax
import jax.numpy as jnp
from jax import lax
from jax.experimental import pallas as pl
from jax.experimental.pallas import tpu as pltpu
from jax.sharding import PartitionSpec as P

TOKEN_CHUNKS = 4
COLUMN_CHUNKS = 8


def last_pieces(depth_w):
    return max(1, min(8, depth_w // 128))


def schedule(token_chunks, column_chunks, col_count):
    events = []
    for t in range(token_chunks):
        for d in range(1, col_count):
            at = (col_count - 1) * t + (1 if d == 1 else d + 1)
            events.append((at, 0, t, d))
    span = (col_count - 1) * token_chunks * 4 / 3
    for j in range(column_chunks - 1):
        events.append((span * (j + 1) / column_chunks, 1, j, 0))
    ordered, clock = [], 0
    for at, kind, first, second in sorted(events, key=lambda e: (e[1], e[2], e[3])):
        if kind == 0:
            clock = max(clock, at)
            at = clock
        ordered.append((at, kind, first, second))
    return sorted(ordered)


def kernel(rows, cols, a_ref, w_ref, o_ref, abuf, wbuf, ysend, yrecv, early, loc_a, loc_w, a_recv, a_right, a_left, w_recv, w_send, p_send, y_recv, y_send):
    r, c, l = lax.axis_index("row"), lax.axis_index("col"), lax.axis_index("layer")
    groups = rows // 2
    core, group = lax.rem(r, 2), r // 2
    partner = 2 * group + 1 - core
    tokens, depth_a = a_ref.shape
    depth_w, width = w_ref.shape
    tt, half = tokens // TOKEN_CHUNKS, width // 2
    nc, jh = width // COLUMN_CHUNKS, COLUMN_CHUNKS // 2
    last, cuts = COLUMN_CHUNKS - 1, last_pieces(depth_w)
    pieces = last + cuts

    def piece(p):
        return (p, 0, depth_w) if p < last else (last, (p - last) * depth_w // cuts, depth_w // cuts)

    def peer(g):
        return 2 * lax.rem(group + g + groups, groups) + core

    def a_at(block, t):
        return abuf.at[block, pl.ds(t * tt, tt), :]

    def w_at(row, p):
        j, start, count = piece(p)
        return wbuf.at[j, pl.ds(pl.multiple_of(row * depth_w + start, count), count), :]

    def own_a(t):
        return pltpu.make_async_copy(a_ref.at[pl.ds(t * tt, tt), :], a_at(c, t), loc_a.at[t])

    def own_w(p):
        j, start, count = piece(p)
        side = 1 - l if j < jh else l
        at = pl.multiple_of(side * half + (j % jh) * nc, nc)
        return pltpu.make_async_copy(w_ref.at[pl.ds(start, count), pl.ds(at, nc)], w_at(r, p), loc_w.at[p])

    def a_copy(block, t, to, sems):
        return pltpu.make_async_remote_copy(a_at(block, t), a_at(block, t), sems.at[t, block], a_recv.at[t, block], device_id={"col": to})

    def w_copy(row, j, to, sem):
        return pltpu.make_async_remote_copy(w_at(row, j), w_at(row, j), sem, w_recv.at[j, row], device_id={"row": to})

    def y_copy(t, j):
        rows_t = pl.ds(t * tt, tt)
        return pltpu.make_async_remote_copy(ysend.at[j, rows_t, :], yrecv.at[j, rows_t, :], y_send.at[t, j], y_recv.at[t, j], device_id={"layer": 1 - l})

    def right(block, t):
        return a_copy(block, t, c + 1, a_right)

    def left(block, t):
        return a_copy(block, t, c - 1, a_left)

    for n in range(max(TOKEN_CHUNKS, pieces)):
        if n < pieces:
            own_w(n).start()
        if n < TOKEN_CHUNKS:
            own_a(n).start()

    has_right, has_left = c < cols - 1, c > 0
    barrier = pltpu.get_barrier_semaphore()

    def greet(device_id):
        pl.semaphore_signal(barrier, inc=1, device_id=device_id)

    greet({"row": partner})
    greet({"layer": 1 - l})
    for g in range(1, groups):
        greet({"row": peer(g)})
    pl.when(has_right)(lambda: greet({"col": c + 1}))
    pl.when(has_left)(lambda: greet({"col": c - 1}))
    pl.semaphore_wait(barrier, 1 + groups + has_right.astype(jnp.int32) + has_left.astype(jnp.int32))

    def send_a(t):
        own_a(t).wait()
        pl.when(has_right)(lambda: right(c, t).start())
        pl.when(has_left)(lambda: left(c, t).start())

    def send_w(j):
        own_w(j).wait()
        for g in range(1, groups):
            w_copy(r, j, peer(g), w_send.at[j, g]).start()
        w_copy(r, j, partner, p_send.at[j, 0]).start()

    send_w(0)
    send_a(0)
    send_a(1)
    for p in range(1, pieces):
        send_w(p)

    def take_a(t, d):
        @pl.when(c >= d)
        def _():
            right(c - d, t).wait_recv()
            pl.when(has_right)(lambda: right(c - d, t).start())

        @pl.when(c + d < cols)
        def _():
            left(c + d, t).wait_recv()
            pl.when(has_left)(lambda: left(c + d, t).start())

        if d == cols - 1 and t + 2 < TOKEN_CHUNKS:
            send_a(t + 2)

    def take_w(j):
        for g in range(1, groups):
            source = peer(-g)
            w_copy(source, j, partner, p_send.at[j, g]).wait_recv()
            w_copy(source, j, partner, p_send.at[j, g]).start()

    def take_partner(j):
        for g in range(groups):
            source = 2 * g + 1 - core
            w_copy(source, j, partner, p_send.at[j, 0]).wait_recv()

    def product(rows_t, j):
        total = jnp.dot(abuf[0, rows_t, :], wbuf[j, pl.ds(0, depth_a), :], preferred_element_type=jnp.float32)
        for block in range(1, cols):
            total += jnp.dot(abuf[block, rows_t, :], wbuf[j, pl.ds(block * depth_a, depth_a), :], preferred_element_type=jnp.float32)
        return total

    def partials(tiles):
        t0, j0 = tiles[0]
        wide = 1 + tiles[-1][1] - j0

        def one(n, carry):
            t, j = t0 + n // wide, j0 + lax.rem(n, wide)
            rows_t = pl.ds(pl.multiple_of(t * tt, tt), tt)
            ysend[j, rows_t, :] = product(rows_t, j)
            return carry

        def send(n, carry):
            y_copy(t0 + n // wide, j0 + lax.rem(n, wide)).start()
            return carry

        lax.fori_loop(0, len(tiles), one, 0)
        lax.fori_loop(0, len(tiles), send, 0)

    def finish(j):
        def one(t, carry):
            rows_t = pl.ds(pl.multiple_of(t * tt * 2, tt * 2), tt * 2)
            y_copy(2 * t, j - jh).wait_recv()
            y_copy(2 * t + 1, j - jh).wait_recv()
            o_ref[rows_t, (j - jh) * nc:(j - jh + 1) * nc] = (product(rows_t, j) + yrecv[j - jh, rows_t, :]).astype(o_ref.dtype)
            return carry

        lax.fori_loop(0, TOKEN_CHUNKS // 2, one, 0)

    def part(j, rows_t, start, count):
        columns = pl.ds(pl.multiple_of(lax.rem(start, depth_a), min(count, depth_a)), count)
        weights = wbuf[j, pl.ds(pl.multiple_of(start, count), count), :]
        return jnp.dot(abuf[start // depth_a, rows_t, columns], weights, preferred_element_type=jnp.float32)

    def each_rows(body):
        def one(t, carry):
            body(pl.ds(pl.multiple_of(t * tt * 2, tt * 2), tt * 2))
            return carry

        lax.fori_loop(0, TOKEN_CHUNKS // 2, one, 0)

    def take_own_rows():
        for h in range(cuts):
            w_copy(partner, last + h, partner, p_send.at[last + h, 0]).wait_recv()
        count = min(depth_w, depth_a)
        for n in range(depth_w // count):
            @each_rows
            def _(rows_t):
                total = part(last, rows_t, r * depth_w + n * count, count) + part(last, rows_t, partner * depth_w + n * count, count)
                early[rows_t, :] = total if n == 0 else early[rows_t, :] + total

    def finish_last():
        count = depth_w // cuts
        for t in range(TOKEN_CHUNKS):
            y_copy(t, jh - 1).wait_recv()
        for h in range(cuts):
            take_w(last + h)
            for g in range(1, groups):
                own, other = peer(-g), peer(-g) + 1 - 2 * core

                @each_rows
                def _(rows_t):
                    early[rows_t, :] += part(last, rows_t, own * depth_w + h * count, count)

                w_copy(other, last + h, partner, p_send.at[last + h, 0]).wait_recv()

                @each_rows
                def _(rows_t):
                    total = early[rows_t, :] + part(last, rows_t, other * depth_w + h * count, count)
                    if h < cuts - 1 or g < groups - 1:
                        early[rows_t, :] = total
                    else:
                        o_ref[rows_t, (jh - 1) * nc:jh * nc] = (total + yrecv[jh - 1, rows_t, :]).astype(o_ref.dtype)

    got_t, got_j, done_own, own_rows = 0, 0, jh, False
    for _, kind, first, second in schedule(TOKEN_CHUNKS, COLUMN_CHUNKS, cols):
        if kind == 0:
            take_a(first, second)
            if second == cols - 1:
                got_t = first + 1
                if got_j:
                    partials([(first, j) for j in range(min(got_j, jh))])
        else:
            if first == last - 1 and got_t == TOKEN_CHUNKS:
                take_own_rows()
                own_rows = True
            take_w(first)
            take_partner(first)
            got_j = first + 1
            if first < jh and got_t:
                partials([(t, first) for t in range(got_t)])
        while got_t == TOKEN_CHUNKS and done_own < got_j:
            finish(done_own)
            done_own += 1
    if not own_rows:
        take_own_rows()
    finish_last()

    for t in range(TOKEN_CHUNKS):
        for block in range(cols):
            @pl.when(has_right & (block <= c))
            def _():
                right(block, t).wait_send()

            @pl.when(has_left & (block >= c))
            def _():
                left(block, t).wait_send()

        for j in range(jh):
            y_copy(t, j).wait_send()
    for p in range(pieces):
        for g in range(groups):
            w_copy(r, p, partner, p_send.at[p, g]).wait_send()
            if g:
                w_copy(r, p, partner, w_send.at[p, g]).wait_send()


def solution(mesh):
    rows, cols = mesh.shape["row"], mesh.shape["col"]

    def shards(attn_values, out_weight):
        tokens, depth_a = attn_values.shape
        depth_w, width = out_weight.shape
        nc, jh = width // COLUMN_CHUNKS, COLUMN_CHUNKS // 2
        pieces = COLUMN_CHUNKS - 1 + last_pieces(depth_w)
        dma = pltpu.SemaphoreType.DMA
        return pl.pallas_call(
            functools.partial(kernel, rows, cols),
            out_shape=jax.ShapeDtypeStruct((tokens, width // 2), jnp.bfloat16),
            in_specs=[pl.BlockSpec(memory_space=pltpu.HBM)] * 2,
            out_specs=pl.BlockSpec(memory_space=pltpu.VMEM),
            scratch_shapes=[
                pltpu.VMEM((cols, tokens, depth_a), jnp.bfloat16),
                pltpu.VMEM((COLUMN_CHUNKS, rows * depth_w, nc), jnp.bfloat16),
                pltpu.VMEM((jh, tokens, nc), jnp.float32),
                pltpu.VMEM((jh, tokens, nc), jnp.float32),
                pltpu.VMEM((tokens, nc), jnp.float32),
                dma((TOKEN_CHUNKS,)),
                dma((pieces,)),
                dma((TOKEN_CHUNKS, cols)),
                dma((TOKEN_CHUNKS, cols)),
                dma((TOKEN_CHUNKS, cols)),
                dma((pieces, rows)),
                dma((pieces, rows // 2)),
                dma((pieces, rows // 2)),
                dma((TOKEN_CHUNKS, jh)),
                dma((TOKEN_CHUNKS, jh)),
            ],
            compiler_params=pltpu.CompilerParams(collective_id=0, has_side_effects=True, vmem_limit_bytes=48 * 2**20),
        )(*(pltpu.with_memory_space_constraint(x, pltpu.HBM) for x in (attn_values, out_weight)))

    in_specs = (P("row", ("layer", "col")), P(("layer", "row"), "col"))
    out_specs = P("row", ("col", "layer"))
    return jax.shard_map(shards, mesh=mesh, in_specs=in_specs, out_specs=out_specs, check_vma=False)
```
